32 devices in a mesh: cp: 16 (over z, x, core), tp: 2 (over y).
Axes of the slice: x: 2, y: 2, z: 4, core: 2. Of those that a mesh axis runs over, the one named last changes fastest.
Arguments:
- query: bfloat16 [1024, 16384], P(('cp', 'tp')), may hold values from -6 to 6
- fresh_key_rows: bfloat16 [1024, 1024], P(('cp', 'tp')), may hold values from -6 to 6
- fresh_value_rows: bfloat16 [1024, 1024], P(('cp', 'tp')), may hold values from -6 to 6
- cached_key_rows: bfloat16 [8192, 1024], P('cp', 'tp'), may hold values from -6 to 6
- cached_value_rows: bfloat16 [8192, 1024], P('cp', 'tp'), may hold values from -6 to 6
- prefix_len: int32 [1], replicated, may hold values from 4096 to 8192
- stripe_owner: int32 [16], replicated, may hold values from 0 to 15, each once
Outputs:
- attended: bfloat16 [1024, 16384], P('cp', 'tp')
The draws below stay inside these ranges and needn't reach their ends.
Inputs may be any that keep to these rules, and one draw needn't show every extreme that they name: `stripe_owner`: a permutation of 0 to 15.
All inputs are finite; a program needn't handle non-finite values.
Results may differ from the reference program's by a relative error of at most 0.0075.
Values may be sent and summed in bfloat16 or wider, within the bound.
A program may use at most 64 MiB of HBM per device.

```python
import math
import jax
import jax.numpy as jnp
from jax import lax

QUERY_HEADS = 128
KEY_VALUE_HEADS = 8
HEAD_SIZE = 128
TOK_DEV = 64
NEW_TOKENS = 1024
CACHE_SLOTS = 8192
N_CP = 16


def draw_query(key, part):
    base_offset = jnp.clip(jax.random.normal(jax.random.fold_in(key, 11), (NEW_TOKENS, QUERY_HEADS * HEAD_SIZE), jnp.float32), -6.0, 6.0)
    return base_offset.astype(jnp.bfloat16)


def draw_cached_key_rows(key, part):
    base_offset = jnp.clip(jax.random.normal(jax.random.fold_in(key, 12), (CACHE_SLOTS, KEY_VALUE_HEADS * HEAD_SIZE), jnp.float32), -6.0, 6.0)
    return base_offset.astype(jnp.bfloat16)


def level_of(rng, extent, shards, low, largest):
    def one(dim, parts):
        heights = jax.random.uniform(jax.random.fold_in(jax.random.fold_in(rng, 6), dim), (parts,), jnp.float32, low / len(shards), largest / len(shards))
        return jnp.repeat(jnp.exp(heights), extent[dim] // parts).reshape((-1,) + (1,) * (len(extent) - dim - 1))

    gain = one(*shards[0])
    for cut in shards[1:]:
        gain = gain * one(*cut)
    return gain


def bell_draw(key, shape, width, most, shards=(), kind=jnp.bfloat16):
    values = jax.random.normal(key, shape, jnp.float32) * width
    if len(shards) > 0:
        values = level_of(key, shape, shards, -0.22, 0.18) * values
    return jnp.clip(values, min=-most, max=most).astype(kind)


def setup_inputs(seed: int = 0) -> dict:
    seeds = jax.random.split(jax.random.key(seed), 8)
    query = draw_query(jax.random.fold_in(seeds[7], 71), 0)
    fresh_key_rows = bell_draw(seeds[1], (NEW_TOKENS, KEY_VALUE_HEADS * HEAD_SIZE), 1.0, 6.0, ((0, 32),))
    fresh_value_rows = bell_draw(seeds[2], (NEW_TOKENS, KEY_VALUE_HEADS * HEAD_SIZE), 1.0, 6.0, ((0, 32),))
    cached_key_rows = draw_cached_key_rows(jax.random.fold_in(seeds[7], 71), 0)
    cached_value_rows = bell_draw(seeds[4], (CACHE_SLOTS, KEY_VALUE_HEADS * HEAD_SIZE), 1.0, 6.0, ((0, 16), (1, 2)))
    prefix_len = jax.random.randint(seeds[5], (1,), CACHE_SLOTS // 2, CACHE_SLOTS + 1).astype(jnp.int32)
    stripe_owner = jax.random.permutation(seeds[6], N_CP).astype(jnp.int32)
    return {"query": query, "fresh_key_rows": fresh_key_rows, "fresh_value_rows": fresh_value_rows, "cached_key_rows": cached_key_rows, "cached_value_rows": cached_value_rows, "prefix_len": prefix_len, "stripe_owner": stripe_owner}


NEG = -1.0e30


def reference(query, fresh_key_rows, fresh_value_rows, cached_key_rows, cached_value_rows, prefix_len, stripe_owner):
    group_size = QUERY_HEADS // KEY_VALUE_HEADS
    scale = HEAD_SIZE ** -0.5
    plen = prefix_len[0]
    block_number = math.gcd(NEW_TOKENS, 256)
    block_count = NEW_TOKENS // block_number
    cache_live = jnp.arange(CACHE_SLOTS, dtype=jnp.int32) < plen
    new_index = jnp.arange(NEW_TOKENS, dtype=jnp.int32)
    combined_keys = jnp.concatenate([cached_key_rows.reshape(CACHE_SLOTS, KEY_VALUE_HEADS, HEAD_SIZE), fresh_key_rows.reshape(NEW_TOKENS, KEY_VALUE_HEADS, HEAD_SIZE)], axis=0).transpose(1, 0, 2)
    combined_values = jnp.concatenate([cached_value_rows.reshape(CACHE_SLOTS, KEY_VALUE_HEADS, HEAD_SIZE), fresh_value_rows.reshape(NEW_TOKENS, KEY_VALUE_HEADS, HEAD_SIZE)], axis=0).transpose(1, 0, 2)
    query_head_rows = query.reshape(block_count, block_number, KEY_VALUE_HEADS, group_size, HEAD_SIZE).transpose(2, 0, 1, 3, 4)

    def per_head(inputs):
        queries, keys, values = inputs
        keys32 = keys.astype(jnp.float32)
        values32 = values.astype(jnp.float32)

        def per_block(pair):
            rows, number = pair
            query_index = number * block_number + jnp.arange(block_number, dtype=jnp.int32)
            scores = jnp.einsum("qgd,kd->gqk", rows.astype(jnp.float32), keys32) * scale
            visible = jnp.concatenate([jnp.broadcast_to(cache_live[None, :], (block_number, CACHE_SLOTS)), new_index[None, :] <= query_index[:, None]], axis=1)
            peak = jnp.max(jnp.where(visible, scores, NEG), axis=-1, keepdims=True)
            weights = jnp.where(visible, jnp.exp(scores - peak), 0.0)
            total = jnp.sum(weights, axis=-1, keepdims=True)
            rounded = lax.optimization_barrier(weights.astype(jnp.bfloat16)).astype(jnp.float32)
            result = jnp.einsum("gqk,kd->gqd", rounded, values32) / total
            return result.astype(jnp.bfloat16)

        return lax.map(per_block, (queries, jnp.arange(block_count, dtype=jnp.int32)))

    outputs = lax.map(per_head, (query_head_rows, combined_keys, combined_values))
    natural = outputs.transpose(1, 3, 0, 2, 4).reshape(NEW_TOKENS, QUERY_HEADS * HEAD_SIZE)
    inverse = jnp.argsort(stripe_owner).astype(jnp.int32)
    stripe = TOK_DEV // N_CP
    arranged = natural.reshape(N_CP, N_CP, stripe, QUERY_HEADS * HEAD_SIZE)[:, inverse]
    return arranged.transpose(1, 0, 2, 3).reshape(NEW_TOKENS, QUERY_HEADS * HEAD_SIZE)
```

```python
import functools
import math

import jax
import jax.numpy as jnp
from jax import lax
from jax.experimental import pallas as pl
from jax.experimental.pallas import tpu as pltpu
from jax.sharding import PartitionSpec as P

HEAD_SIZE = 128
NEG = -1e30
EXPONENT = HEAD_SIZE ** (-0.5) * math.log2(math.e)


def attend_kernel(
    dims,
    plen_ref,
    q_ref,
    nat_ref,
    fresh_k,
    fresh_v,
    cache_k,
    cache_v,
    out_ref,
    m_ref,
    l_ref,
    acc_ref,
):
    per_step, chunk, fresh_chunk = dims
    rows = q_ref.shape[0]
    slots = cache_k.shape[0]
    plen = plen_ref[0]

    def piece(g, k, v, mask, first):
        q = q_ref[:, g * HEAD_SIZE : (g + 1) * HEAD_SIZE]
        s = lax.dot_general(q, k, (((1,), (1,)), ((), ())), preferred_element_type=jnp.float32)
        if mask is not None:
            s = jnp.where(mask, s, NEG)
        top = jnp.max(s, axis=1, keepdims=True)
        if first:
            m_new = jnp.broadcast_to(top, (rows, HEAD_SIZE))
        else:
            m_old = m_ref[g]
            m_new = jnp.maximum(m_old, top)
        p = jnp.exp2((s - m_new[:, :1]) * EXPONENT)
        part = p[:, :HEAD_SIZE]
        for c in range(1, p.shape[1] // HEAD_SIZE):
            part = part + p[:, c * HEAD_SIZE : (c + 1) * HEAD_SIZE]
        o = jnp.dot(p.astype(jnp.bfloat16), v, preferred_element_type=jnp.float32)
        m_ref[g] = m_new
        if first:
            l_ref[g] = part
            acc_ref[g] = o
        else:
            f = jnp.exp2((m_old - m_new) * EXPONENT)
            l_ref[g] = f * l_ref[g] + part
            acc_ref[g] = f * acc_ref[g] + o

    fresh = fresh_k.shape[0]
    for c in range(fresh // fresh_chunk):
        k = fresh_k[c * fresh_chunk : (c + 1) * fresh_chunk, :]
        v = fresh_v[c * fresh_chunk : (c + 1) * fresh_chunk, :]
        index = c * fresh_chunk + lax.broadcasted_iota(jnp.int32, (rows, fresh_chunk), 1)
        mask = index <= nat_ref[:, :1]
        for g in range(per_step):
            piece(g, k, v, mask, c == 0)

    def body(b, _):
        at = pl.multiple_of(b * chunk, chunk)
        k = cache_k[pl.ds(at, chunk), :]
        v = cache_v[pl.ds(at, chunk), :]
        for g in range(per_step):
            piece(g, k, v, None, False)
        return 0

    full = plen // chunk
    lax.fori_loop(0, full, body, 0)

    @pl.when(full * chunk < plen)
    def _():
        at = pl.multiple_of(full * chunk, chunk)
        k = cache_k[pl.ds(at, chunk), :]
        v = cache_v[pl.ds(at, chunk), :]
        index = at + lax.broadcasted_iota(jnp.int32, (1, chunk), 1)
        for g in range(per_step):
            piece(g, k, v, index < plen, False)

    for g in range(per_step):
        total = jnp.sum(l_ref[g], axis=1, keepdims=True)
        out_ref[:, g * HEAD_SIZE : (g + 1) * HEAD_SIZE] = (acc_ref[g] / total).astype(out_ref.dtype)


def attend(q, nat, fresh_k, fresh_v, cache_k, cache_v, prefix_len, per_step=4, chunk=1024):
    rows, columns = q.shape
    width = per_step * HEAD_SIZE
    fresh, slots = fresh_k.shape[0], cache_k.shape[0]
    whole = lambda i, *_: (0, 0)
    flops = 4 * rows * columns * (fresh + slots)
    return pl.pallas_call(
        functools.partial(attend_kernel, (per_step, min(chunk, slots), min(chunk, fresh))),
        out_shape=jax.ShapeDtypeStruct((rows, columns), jnp.bfloat16),
        grid_spec=pltpu.PrefetchScalarGridSpec(
            num_scalar_prefetch=1,
            grid=(columns // width,),
            in_specs=[
                pl.BlockSpec((rows, width), lambda i, *_: (0, i)),
                pl.BlockSpec((rows, HEAD_SIZE), whole),
                pl.BlockSpec((fresh, HEAD_SIZE), whole),
                pl.BlockSpec((fresh, HEAD_SIZE), whole),
                pl.BlockSpec((slots, HEAD_SIZE), whole),
                pl.BlockSpec((slots, HEAD_SIZE), whole),
            ],
            out_specs=pl.BlockSpec((rows, width), lambda i, *_: (0, i)),
            scratch_shapes=[pltpu.VMEM((per_step, rows, HEAD_SIZE), jnp.float32)] * 3,
        ),
        compiler_params=pltpu.CompilerParams(vmem_limit_bytes=56 * 1024 * 1024),
        cost_estimate=pl.CostEstimate(
            flops=flops, bytes_accessed=4 * fresh * columns, transcendentals=0
        ),
    )(prefix_len, q, nat, fresh_k, fresh_v, cache_k, cache_v)


def shards(
    query,
    fresh_key_rows,
    fresh_value_rows,
    cached_key_rows,
    cached_value_rows,
    prefix_len,
    stripe_owner,
):
    parts = lax.axis_size("cp")
    tps = lax.axis_size("tp")
    me = lax.axis_index("cp")
    heads = cached_key_rows.shape[1] // HEAD_SIZE
    ranks = parts // heads
    q_columns = query.shape[1] // tps // heads
    columns = [[h * ranks + r for h in range(heads)] for r in range(ranks)]
    lines = [[h * ranks + r for r in range(ranks)] for h in range(heads)]

    order = jnp.arange(parts, dtype=jnp.int32)
    inverse = jnp.sum(jnp.where(stripe_owner[None, :] == order[:, None], order[None, :], 0), axis=1)

    def split_heads(array):
        if heads == 1:
            return array
        return lax.all_to_all(
            array, "cp", split_axis=1, concat_axis=0, axis_index_groups=columns, tiled=True
        )

    def collect(array):
        block = array.shape[0]
        mine = split_heads(array)
        everything = lax.all_gather(mine, "cp", axis_index_groups=lines, tiled=True)
        return (
            everything.reshape(ranks, heads, block, HEAD_SIZE)
            .transpose(1, 0, 2, 3)
            .reshape(parts * block, HEAD_SIZE)
        )

    q_local = lax.all_to_all(query, "tp", split_axis=1, concat_axis=0, tiled=True)
    fresh = jnp.concatenate(
        [
            fresh_key_rows.reshape(-1, tps, heads, 1, HEAD_SIZE),
            fresh_value_rows.reshape(-1, tps, heads, 1, HEAD_SIZE),
        ],
        axis=3,
    ).reshape(fresh_key_rows.shape[0], -1)
    f_local = lax.all_to_all(fresh, "tp", split_axis=1, concat_axis=0, tiled=True)
    rows = q_local.shape[0]
    stripe = rows // parts

    by_rank = inverse.reshape(heads, ranks).T.reshape(-1)
    wanted = (by_rank[:, None] * stripe + jnp.arange(stripe, dtype=jnp.int32)[None, :]).reshape(-1)
    pick = (wanted[:, None] == jnp.arange(rows, dtype=jnp.int32)[None, :]).astype(jnp.bfloat16)
    q_sorted = jnp.dot(pick, q_local, preferred_element_type=jnp.float32).astype(jnp.bfloat16)
    q_out = (
        q_sorted.reshape(ranks, heads * stripe, heads, q_columns)
        .transpose(2, 0, 1, 3)
        .reshape(parts * heads * stripe, q_columns)
    )
    q_mine = lax.all_to_all(q_out, "cp", split_axis=0, concat_axis=0, tiled=True)

    cache_k = collect(cached_key_rows)
    cache_v = collect(cached_value_rows)
    if heads > 1:
        f_mine = lax.all_to_all(
            f_local, "cp", split_axis=1, concat_axis=0, axis_index_groups=columns, tiled=True
        )
    else:
        f_mine = f_local
    f_all = lax.all_gather(f_mine, "cp", axis_index_groups=lines, tiled=True)
    f_all = (
        f_all.reshape(ranks, heads, rows, 2 * HEAD_SIZE)
        .transpose(1, 0, 2, 3)
        .reshape(parts * rows, 2 * HEAD_SIZE)
    )
    fresh_k, fresh_v = f_all[:, :HEAD_SIZE], f_all[:, HEAD_SIZE:]

    rank = me % ranks
    residues = jnp.take(by_rank.reshape(ranks, heads), rank, axis=0)
    nat = (
        jnp.arange(parts, dtype=jnp.int32)[:, None, None] * rows
        + residues[None, :, None] * stripe
        + jnp.arange(stripe, dtype=jnp.int32)[None, None, :]
    ).reshape(-1, 1)
    nat = jnp.broadcast_to(nat, (nat.shape[0], HEAD_SIZE))

    done = attend(q_mine, nat, fresh_k, fresh_v, cache_k, cache_v, prefix_len)
    done = (
        done.reshape(parts, heads, stripe, q_columns)
        .transpose(1, 0, 2, 3)
        .reshape(heads * rows, q_columns)
    )
    if heads == 1:
        return done
    return lax.all_to_all(
        done, "cp", split_axis=0, concat_axis=1, axis_index_groups=columns, tiled=True
    )


def solution(mesh):
    return jax.shard_map(
        shards,
        mesh=mesh,
        in_specs=(
            P(("cp", "tp"), None),
            P(("cp", "tp"), None),
            P(("cp", "tp"), None),
            P("cp", "tp"),
            P("cp", "tp"),
            P(),
            P(),
        ),
        out_specs=P("cp", "tp"),
        check_vma=False,
    )
```

```python
import functools
import math

import jax
import jax.numpy as jnp
from jax import lax
from jax.experimental import pallas as pl
from jax.experimental.pallas import tpu as pltpu
from jax.sharding import PartitionSpec as P

HEAD_SIZE = 128
NEG = -1e30
EXPONENT = HEAD_SIZE ** (-0.5) * math.log2(math.e)


def attend_kernel(
    dims,
    plen_ref,
    q_ref,
    nat_ref,
    fresh_k,
    fresh_v,
    cache_k,
    cache_v,
    out_ref,
    m_ref,
    acc_ref,
    fresh_x,
    cache_x,
):
    per_step, chunk, fresh_chunk = dims
    rows = q_ref.shape[0]
    plen = plen_ref[0]

    @pl.when(pl.program_id(0) == 0)
    def _():
        for plain, wide in ((fresh_v, fresh_x), (cache_v, cache_x)):
            wide[:, :HEAD_SIZE] = plain[...]
            wide[:, HEAD_SIZE:] = jnp.ones(plain.shape, jnp.bfloat16)

    def piece(g, k, v, mask, first):
        q = q_ref[:, g * HEAD_SIZE : (g + 1) * HEAD_SIZE]
        s = lax.dot_general(q, k, (((1,), (1,)), ((), ())), preferred_element_type=jnp.float32)
        if mask is not None:
            s = jnp.where(mask, s, NEG)
        top = jnp.max(s, axis=1, keepdims=True)
        if first:
            m_new = jnp.broadcast_to(top, (rows, HEAD_SIZE))
        else:
            m_old = m_ref[g]
            m_new = jnp.maximum(m_old, top)
        p = jnp.exp2((s - m_new[:, :1]) * EXPONENT)
        o = jnp.dot(p.astype(jnp.bfloat16), v, preferred_element_type=jnp.float32)
        m_ref[g] = m_new
        if first:
            acc_ref[g] = o
        else:
            f = jnp.exp2((m_old - m_new) * EXPONENT)
            acc_ref[g, :, :HEAD_SIZE] = f * acc_ref[g, :, :HEAD_SIZE] + o[:, :HEAD_SIZE]
            acc_ref[g, :, HEAD_SIZE:] = f * acc_ref[g, :, HEAD_SIZE:] + o[:, HEAD_SIZE:]

    fresh = fresh_k.shape[0]
    for c in range(fresh // fresh_chunk):
        k = fresh_k[c * fresh_chunk : (c + 1) * fresh_chunk, :]
        v = fresh_x[c * fresh_chunk : (c + 1) * fresh_chunk, :]
        index = c * fresh_chunk + lax.broadcasted_iota(jnp.int32, (rows, fresh_chunk), 1)
        mask = index <= nat_ref[:, :1]
        for g in range(per_step):
            piece(g, k, v, mask, c == 0)

    def body(b, _):
        at = pl.multiple_of(b * chunk, chunk)
        k = cache_k[pl.ds(at, chunk), :]
        v = cache_x[pl.ds(at, chunk), :]
        for g in range(per_step):
            piece(g, k, v, None, False)
        return 0

    full = plen // chunk
    lax.fori_loop(0, full, body, 0)

    @pl.when(full * chunk < plen)
    def _():
        at = pl.multiple_of(full * chunk, chunk)
        k = cache_k[pl.ds(at, chunk), :]
        v = cache_x[pl.ds(at, chunk), :]
        index = at + lax.broadcasted_iota(jnp.int32, (1, chunk), 1)
        for g in range(per_step):
            piece(g, k, v, index < plen, False)

    for g in range(per_step):
        out_ref[:, g * HEAD_SIZE : (g + 1) * HEAD_SIZE] = (
            acc_ref[g, :, :HEAD_SIZE] / acc_ref[g, :, HEAD_SIZE:]
        ).astype(out_ref.dtype)


def attend(q, nat, fresh_k, fresh_v, cache_k, cache_v, prefix_len, per_step=4, chunk=1024):
    rows, columns = q.shape
    width = per_step * HEAD_SIZE
    fresh, slots = fresh_k.shape[0], cache_k.shape[0]
    whole = lambda i, *_: (0, 0)
    flops = 4 * rows * columns * (fresh + slots)
    return pl.pallas_call(
        functools.partial(attend_kernel, (per_step, min(chunk, slots), min(chunk, fresh))),
        out_shape=jax.ShapeDtypeStruct((rows, columns), jnp.bfloat16),
        grid_spec=pltpu.PrefetchScalarGridSpec(
            num_scalar_prefetch=1,
            grid=(columns // width,),
            in_specs=[
                pl.BlockSpec((rows, width), lambda i, *_: (0, i)),
                pl.BlockSpec((rows, HEAD_SIZE), whole),
                pl.BlockSpec((fresh, HEAD_SIZE), whole),
                pl.BlockSpec((fresh, HEAD_SIZE), whole),
                pl.BlockSpec((slots, HEAD_SIZE), whole),
                pl.BlockSpec((slots, HEAD_SIZE), whole),
            ],
            out_specs=pl.BlockSpec((rows, width), lambda i, *_: (0, i)),
            scratch_shapes=[
                pltpu.VMEM((per_step, rows, HEAD_SIZE), jnp.float32),
                pltpu.VMEM((per_step, rows, 2 * HEAD_SIZE), jnp.float32),
                pltpu.VMEM((fresh, 2 * HEAD_SIZE), jnp.bfloat16),
                pltpu.VMEM((slots, 2 * HEAD_SIZE), jnp.bfloat16),
            ],
        ),
        compiler_params=pltpu.CompilerParams(vmem_limit_bytes=56 * 1024 * 1024),
        cost_estimate=pl.CostEstimate(
            flops=flops, bytes_accessed=4 * fresh * columns, transcendentals=0
        ),
    )(prefix_len, q, nat, fresh_k, fresh_v, cache_k, cache_v)


def remote(source, target, send, receive, device):
    return pltpu.make_async_remote_copy(
        src_ref=source,
        dst_ref=target,
        send_sem=send,
        recv_sem=receive,
        device_id=device,
        device_id_type=pl.DeviceIdType.MESH,
    )


def greet(devices):
    barrier = pltpu.get_barrier_semaphore()
    for device in devices:
        pl.semaphore_signal(
            barrier, inc=1, device_id=device, device_id_type=pl.DeviceIdType.MESH
        )
    pl.semaphore_wait(barrier, len(devices))


def collect_kernel(
    heads,
    ranks,
    tps,
    cache_k,
    cache_v,
    fresh_k,
    fresh_v,
    all_ck,
    all_cv,
    all_fk,
    all_fv,
    local_k,
    local_v,
    tp_send,
    tp_recv,
    own_sem,
    z_send,
    z_recv,
    *rank_sems,
):
    me, tp = lax.axis_index("cp"), lax.axis_index("tp")
    row, rank = me // ranks, me % ranks
    arrays = ((cache_k, all_ck), (cache_v, all_cv), (local_k, all_fk), (local_v, all_fv))
    bits = []
    bit = ranks // 2
    while bit:
        bits.append(bit)
        bit //= 2
    partners = [rank + bit - 2 * bit * ((rank // bit) % 2) for bit in bits]
    column = [{"cp": (row + s) % heads * ranks + rank} for s in range(heads)]
    line = [{"cp": row * ranks + partner} for partner in partners]
    greet(column[1:] + line + [{"tp": (tp + t) % tps} for t in range(1, tps)])

    def cut(ref, head):
        return ref.at[:, pl.ds(pl.multiple_of(head * HEAD_SIZE, HEAD_SIZE), HEAD_SIZE)]

    def place(ref, index):
        block = ref.shape[0] // (heads * ranks)
        return ref.at[pl.ds(pl.multiple_of(index * block, block), block), :]

    started = []

    def go(copy):
        copy.start()
        started.append(copy)
        return copy

    def scatter(a):
        source, target = arrays[a]
        own = pltpu.make_async_copy(cut(source, row), place(target, me), own_sem.at[a])
        own.start()
        copies = [own]
        for s in range(1, heads):
            copies.append(
                go(
                    remote(
                        cut(source, (row + s) % heads),
                        place(target, me),
                        z_send.at[a, s],
                        z_recv.at[a, s],
                        column[s],
                    )
                )
            )
        return copies

    wide = heads * HEAD_SIZE
    few = fresh_k.shape[0]
    exchange = []
    for a, (source, target) in enumerate(((fresh_k, local_k), (fresh_v, local_v))):
        mine = target.at[pl.ds(pl.multiple_of(tp * few, few), few), :]
        for t in range(tps):
            to = (tp + t) % tps
            piece = source.at[:, pl.ds(pl.multiple_of(to * wide, wide), wide)]
            if t == 0:
                copy = pltpu.make_async_copy(piece, mine, own_sem.at[4 + a])
                copy.start()
            else:
                copy = go(remote(piece, mine, tp_send.at[a, t], tp_recv.at[a, t], {"tp": to}))
            exchange.append((t, copy))
    scattered = [scatter(0), scatter(1)]
    for t, copy in exchange:
        copy.wait() if t == 0 else copy.wait_recv()
    scattered += [scatter(2), scatter(3)]

    order = (0, 1, 2, 3)
    held = [(a, s, rank) for s in range(heads) for a in order]
    waits = {
        (a, s, 0): (scattered[a][s].wait if s == 0 else scattered[a][s].wait_recv)
        for a in order
        for s in range(heads)
    }
    held = [((a, s, 0), a, s, rank) for s in range(heads) for a in order]
    for level, partner in enumerate(partners):
        send, receive = rank_sems[2 * level], rank_sems[2 * level + 1]
        other = []
        for number, (key, a, s, owner) in enumerate(held):
            if waits.get(key) is not None:
                waits[key]()
                waits[key] = None
            index = (row + heads - s) % heads * ranks + owner
            target = arrays[a][1]
            copy = go(
                remote(
                    place(target, index),
                    place(target, index),
                    send.at[number],
                    receive.at[number],
                    line[level],
                )
            )
            bit = bits[level]
            name = (a, s, level + 1, number)
            waits[name] = copy.wait_recv
            other.append((name, a, s, owner + bit - 2 * bit * ((owner // bit) % 2)))
        held = held + other
    for wait in waits.values():
        if wait is not None:
            wait()
    for copy in started:
        copy.wait_send()


def collect_all(cache_k, cache_v, fresh_k, fresh_v, heads, ranks, tps):
    block, rows = cache_k.shape[0], fresh_k.shape[0] * tps
    wide = heads * HEAD_SIZE
    out = [
        jax.ShapeDtypeStruct((heads * ranks * n, HEAD_SIZE), jnp.bfloat16)
        for n in (block, block, rows, rows)
    ]
    rank_sems = []
    count = 4 * heads
    size = ranks
    while size > 1:
        rank_sems += [pltpu.SemaphoreType.DMA((count,))] * 2
        count *= 2
        size //= 2
    return pl.pallas_call(
        functools.partial(collect_kernel, heads, ranks, tps),
        out_shape=out,
        in_specs=[pl.BlockSpec(memory_space=pltpu.VMEM)] * 4,
        out_specs=[pl.BlockSpec(memory_space=pl.ANY)] * 4,
        scratch_shapes=[
            pltpu.VMEM((rows, wide), jnp.bfloat16),
            pltpu.VMEM((rows, wide), jnp.bfloat16),
            pltpu.SemaphoreType.DMA((2, tps)),
            pltpu.SemaphoreType.DMA((2, tps)),
            pltpu.SemaphoreType.DMA((6,)),
            pltpu.SemaphoreType.DMA((4, heads)),
            pltpu.SemaphoreType.DMA((4, heads)),
        ]
        + rank_sems,
        compiler_params=pltpu.CompilerParams(collective_id=1, has_side_effects=True),
        cost_estimate=pl.CostEstimate(flops=0, bytes_accessed=100000000, transcendentals=0),
    )(cache_k, cache_v, fresh_k, fresh_v)


def return_kernel(heads, ranks, done, out, own_sem, send, receive):
    me = lax.axis_index("cp")
    row, rank = me // ranks, me % ranks
    rows, width = out.shape[0], done.shape[1]
    column = [{"cp": (row + s) % heads * ranks + rank} for s in range(heads)]
    greet(column[1:])
    target = out.at[:, pl.ds(pl.multiple_of(row * width, width), width)]
    copies = []
    for s in list(range(1, heads)) + [0]:
        to = (row + s) % heads
        source = done.at[pl.ds(pl.multiple_of(to * rows, rows), rows), :]
        if s == 0:
            copy = pltpu.make_async_copy(source, target, own_sem)
        else:
            copy = remote(source, target, send.at[s], receive.at[s], column[s])
        copy.start()
        copies.append(copy)
    for copy in copies:
        copy.wait()


def give_back(done, heads, ranks):
    rows = done.shape[0] // heads
    return pl.pallas_call(
        functools.partial(return_kernel, heads, ranks),
        out_shape=jax.ShapeDtypeStruct((rows, heads * done.shape[1]), jnp.bfloat16),
        in_specs=[pl.BlockSpec(memory_space=pltpu.VMEM)],
        out_specs=pl.BlockSpec(memory_space=pltpu.VMEM),
        scratch_shapes=[
            pltpu.SemaphoreType.DMA,
            pltpu.SemaphoreType.DMA((heads,)),
            pltpu.SemaphoreType.DMA((heads,)),
        ],
        compiler_params=pltpu.CompilerParams(collective_id=2, has_side_effects=True),
        cost_estimate=pl.CostEstimate(flops=0, bytes_accessed=30000000, transcendentals=0),
    )(done)


def shards(
    query,
    fresh_key_rows,
    fresh_value_rows,
    cached_key_rows,
    cached_value_rows,
    prefix_len,
    stripe_owner,
):
    parts = lax.axis_size("cp")
    tps = lax.axis_size("tp")
    me = lax.axis_index("cp")
    heads = cached_key_rows.shape[1] // HEAD_SIZE
    ranks = parts // heads
    q_columns = query.shape[1] // tps // heads
    columns = [[h * ranks + r for h in range(heads)] for r in range(ranks)]
    lines = [[h * ranks + r for r in range(ranks)] for h in range(heads)]

    order = jnp.arange(parts, dtype=jnp.int32)
    inverse = jnp.sum(jnp.where(stripe_owner[None, :] == order[:, None], order[None, :], 0), axis=1)

    def split_heads(array):
        if heads == 1:
            return array
        return lax.all_to_all(
            array, "cp", split_axis=1, concat_axis=0, axis_index_groups=columns, tiled=True
        )

    def collect(array):
        block = array.shape[0]
        mine = split_heads(array)
        everything = lax.all_gather(mine, "cp", axis_index_groups=lines, tiled=True)
        return (
            everything.reshape(ranks, heads, block, HEAD_SIZE)
            .transpose(1, 0, 2, 3)
            .reshape(parts * block, HEAD_SIZE)
        )

    q_local = lax.all_to_all(query, "tp", split_axis=1, concat_axis=0, tiled=True)
    rows = q_local.shape[0]
    stripe = rows // parts

    by_rank = inverse.reshape(heads, ranks).T.reshape(-1)
    wanted = (by_rank[:, None] * stripe + jnp.arange(stripe, dtype=jnp.int32)[None, :]).reshape(-1)
    pick = (wanted[:, None] == jnp.arange(rows, dtype=jnp.int32)[None, :]).astype(jnp.bfloat16)
    q_sorted = jnp.dot(pick, q_local, preferred_element_type=jnp.float32).astype(jnp.bfloat16)
    q_out = (
        q_sorted.reshape(ranks, heads * stripe, heads, q_columns)
        .transpose(2, 0, 1, 3)
        .reshape(parts * heads * stripe, q_columns)
    )
    q_mine = lax.all_to_all(q_out, "cp", split_axis=0, concat_axis=0, tiled=True)

    if heads > 1 and ranks & (ranks - 1) == 0:
        cache_k, cache_v, fresh_k, fresh_v = collect_all(
            cached_key_rows, cached_value_rows, fresh_key_rows, fresh_value_rows, heads, ranks, tps
        )
    else:
        own = [
            lax.all_to_all(array, "tp", split_axis=1, concat_axis=0, tiled=True)
            for array in (fresh_key_rows, fresh_value_rows)
        ]
        cache_k, cache_v, fresh_k, fresh_v = (
            collect(array) for array in (cached_key_rows, cached_value_rows, *own)
        )

    rank = me % ranks
    residues = jnp.take(by_rank.reshape(ranks, heads), rank, axis=0)
    nat = (
        jnp.arange(parts, dtype=jnp.int32)[:, None, None] * rows
        + residues[None, :, None] * stripe
        + jnp.arange(stripe, dtype=jnp.int32)[None, None, :]
    ).reshape(-1, 1)
    nat = jnp.broadcast_to(nat, (nat.shape[0], HEAD_SIZE))

    done = attend(q_mine, nat, fresh_k, fresh_v, cache_k, cache_v, prefix_len)
    done = (
        done.reshape(parts, heads, stripe, q_columns)
        .transpose(1, 0, 2, 3)
        .reshape(heads * rows, q_columns)
    )
    if heads == 1:
        return done
    return give_back(done, heads, ranks)


def solution(mesh):
    return jax.shard_map(
        shards,
        mesh=mesh,
        in_specs=(
            P(("cp", "tp"), None),
            P(("cp", "tp"), None),
            P(("cp", "tp"), None),
            P("cp", "tp"),
            P("cp", "tp"),
            P(),
            P(),
        ),
        out_specs=P("cp", "tp"),
        check_vma=False,
    )
```
